256 devices in a mesh: dp: 16 (over x, z_lo), hyper: 16 (over y, z_hi, core).
Axes of the slice: x: 4, y: 4, z: 8 (z_hi: 2, z_lo: 4; z = z_hi * 4 + z_lo), core: 2. Of those that a mesh axis runs over, the one named last changes fastest.
Arguments:
- inputs: bfloat16 [512, 64, 128], P(('dp', 'hyper')), may hold values from -64 to 64
- labels: int32 [512, 64], P(('dp', 'hyper')), may hold values from 0 to 255
- client_ids: int32 [512], P(('dp', 'hyper')), may hold values from 0 to 511
- ext_weight: bfloat16 [128, 4096], replicated, may hold values from -0.5 to 0.5
- ext_bias: bfloat16 [4096], replicated, may hold values from -3 to 3
- embeddings: bfloat16 [512, 128], replicated, may hold values from -1.5 to 1.5
- hyper_in: bfloat16 [128, 50], replicated, may hold values from -2.09375 to 2.09375
- hyper_bias: float32 [50], replicated, may hold values from -3 to 3
- hyper_out: bfloat16 [4096, 50, 256], P('hyper'), may hold values from -0.1796875 to 0.1796875
Outputs:
- grad_ext_weight: float32 [128, 4096], replicated
- grad_ext_bias: float32 [4096], replicated
- grad_embeddings: float32 [512, 128], replicated
- grad_hyper_in: float32 [128, 50], replicated
- grad_hyper_bias: float32 [50], replicated
- grad_hyper_out: float32 [4096, 50, 256], P(('hyper', 'dp'))
The draws below stay inside these ranges and needn't reach their ends.
Inputs may be any that keep to these rules, and one draw needn't show every extreme that they name: `client_ids`: A client may hold several slots or none.
All inputs are finite; a program needn't handle non-finite values.
Results may differ from the reference program's by a relative error of at most 0.014.
The reference program's roundings to bfloat16 on the way count: a program that leaves them out, or rounds other values in their place, can miss the bound.
Values may be sent and summed in bfloat16 or wider, within the bound.
No kernel may reach another device: no remote copies, remote signals or barrier semaphores. Data moves between devices by JAX's collectives and lax.ppermute only.
A program may use at most 128 MiB of HBM per device.

```python
import jax
import jax.numpy as jnp
from jax import lax

D = 4096
C = 256
DIN = 128
HH = 50
E = 128
CD = 2
R = 64
SLOTS = 512
NCL = 512
N_DP = 16
N_HYPER = 16


def draw_inputs(key, part):
    values = jax.random.normal(key, (SLOTS, R, DIN), jnp.float32)
    values = jnp.clip(values, -6.0, 6.0)
    return jnp.clip(values, -64.0, 64.0).astype(jnp.bfloat16)


def with_ends(result, key, low, high):
    shape = result.shape
    place = [jax.random.randint(jax.random.fold_in(key, axis), (), 0, shape[axis]) for axis in range(len(shape))]
    result = result.at[tuple(place)].set(low)
    longest = shape.index(max(shape))
    place[longest] = (place[longest] + 1) % shape[longest]
    return result.at[tuple(place)].set(high)


def block_scale(rng, dims, cuts, smallest, high):
    loudness = 1.0
    for axis_at, shards_of in cuts:
        draws = jax.random.uniform(jax.random.fold_in(jax.random.fold_in(rng, 6), axis_at), (shards_of,), jnp.float32, smallest / len(cuts), high / len(cuts))
        loudness = loudness * jnp.repeat(jnp.exp(draws), dims[axis_at] // shards_of).reshape((-1,) + (1,) * (len(dims) - 1 - axis_at))
    return loudness


def gaussian(own_key, extent, spread, bound, shards=(), kind=jnp.bfloat16):
    loudness = block_scale(own_key, extent, shards, -0.22, 0.18) if shards else 1.0
    array = jax.random.normal(own_key, extent, jnp.float32) * spread * loudness
    return jnp.minimum(jnp.maximum(array, -bound), bound).astype(kind)


def setup_inputs(seed: int = 0) -> dict:
    splits = jax.random.split(jax.random.key(seed), 10)
    return {
        "inputs": draw_inputs(jax.random.fold_in(splits[9], 71), 0),
        "labels": with_ends(jax.random.randint(splits[1], (SLOTS, R), 0, C), jax.random.fold_in(splits[1], 1), 0, C - 1).astype(jnp.int32),
        "client_ids": with_ends(jax.random.randint(splits[2], (SLOTS,), 0, NCL), jax.random.fold_in(splits[2], 1), 0, NCL - 1).astype(jnp.int32),
        "ext_weight": gaussian(splits[3], (DIN, D), DIN ** -0.5, 0.5),
        "ext_bias": gaussian(splits[4], (D,), 0.5, 3.0),
        "embeddings": gaussian(splits[5], (NCL, E), 0.25, 1.5),
        "hyper_in": gaussian(splits[6], (E, HH), 0.35, 2.09375),
        "hyper_bias": gaussian(splits[7], (HH,), 0.5, 3.0, (), jnp.float32),
        "hyper_out": gaussian(splits[8], (D, HH, C), 0.03, 0.1796875, ((0, 16),)),
    }


highest = lax.Precision.HIGHEST


def silu_slope(values):
    logistic = jax.nn.sigmoid(values)
    return logistic * (1.0 + values * (1.0 - logistic))


def class_grads(logits, slot_labels, row_count):
    largest = jnp.max(logits, axis=-1, keepdims=True)
    exponent = jnp.exp(logits - largest)
    probability = exponent / jnp.sum(exponent, axis=-1, keepdims=True)
    classes = jnp.arange(logits.shape[-1], dtype=jnp.int32)
    onehot = (slot_labels[..., None] == classes).astype(jnp.float32)
    return ((probability - onehot) / row_count).astype(jnp.bfloat16)


def reference(inputs, labels, client_ids, ext_weight, ext_bias, embeddings, hyper_in, hyper_bias, hyper_out):
    group_size = N_HYPER * CD
    hyper_wide = hyper_out.astype(jnp.float32)
    hyper_in_wide = hyper_in.astype(jnp.float32)
    client_table = jnp.arange(NCL, dtype=jnp.int32)

    def one_group(totals, group_index):
        first_slot = (group_index * group_size).astype(jnp.int32)
        slot_inputs = lax.dynamic_slice_in_dim(inputs, first_slot, group_size, 0)
        slot_labels = lax.dynamic_slice_in_dim(labels, first_slot, group_size, 0)
        slot_ids = lax.dynamic_slice_in_dim(client_ids, first_slot, group_size, 0)
        flat_in = slot_inputs.reshape(group_size * R, DIN)
        preact = jnp.dot(flat_in, ext_weight, preferred_element_type=jnp.float32) + ext_bias.astype(jnp.float32)
        features = jax.nn.silu(preact).astype(jnp.bfloat16).reshape(group_size, R, D)
        picked = embeddings[slot_ids]
        hyper_preact = jnp.dot(picked, hyper_in, preferred_element_type=jnp.float32) + hyper_bias
        hidden = jax.nn.silu(hyper_preact).astype(jnp.bfloat16)
        client_heads = jnp.einsum("kh,dhc->kdc", hidden.astype(jnp.float32), hyper_wide).astype(jnp.bfloat16)
        feat_wide = features.astype(jnp.float32)
        heads_wide = client_heads.astype(jnp.float32)
        logits = jnp.einsum("krd,kdc->krc", feat_wide, heads_wide)
        dlogits = class_grads(logits, slot_labels, R)
        dlog_wide = dlogits.astype(jnp.float32)
        dheads = jnp.einsum("krd,krc->kdc", feat_wide, dlog_wide).astype(jnp.bfloat16)
        dfeatures = jnp.einsum("krc,kdc->krd", dlog_wide, heads_wide).astype(jnp.bfloat16)
        dpreact = (dfeatures.reshape(group_size * R, D).astype(jnp.float32) * silu_slope(preact)).astype(jnp.bfloat16)
        grad_weight = jnp.dot(flat_in.T, dpreact, preferred_element_type=jnp.float32)
        grad_bias = jnp.sum(dpreact.astype(jnp.float32), axis=0)
        dheads_wide = dheads.astype(jnp.float32)
        group_out = jnp.einsum("kh,kdc->dhc", hidden.astype(jnp.float32), dheads_wide)
        group_out = lax.optimization_barrier(group_out.astype(jnp.bfloat16)).astype(jnp.float32)
        dhidden = jnp.einsum("kdc,dhc->kh", dheads_wide, hyper_wide)
        hyper_dpre = dhidden * silu_slope(hyper_preact)
        grad_in = jnp.dot(picked.astype(jnp.float32).T, hyper_dpre, precision=highest)
        grad_hbias = jnp.sum(hyper_dpre, axis=0)
        select = (slot_ids[:, None] == client_table[None, :]).astype(jnp.float32)
        grad_table = jnp.dot(select.T, jnp.dot(hyper_dpre, hyper_in_wide.T, precision=highest), precision=highest)
        updated = (totals[0] + grad_weight, totals[1] + grad_bias, totals[2] + grad_table,
                   totals[3] + grad_in, totals[4] + grad_hbias, totals[5] + group_out)
        return updated, None

    initial = (jnp.zeros((DIN, D), jnp.float32), jnp.zeros((D,), jnp.float32), jnp.zeros((NCL, E), jnp.float32),
               jnp.zeros((E, HH), jnp.float32), jnp.zeros((HH,), jnp.float32), jnp.zeros((D, HH, C), jnp.float32))
    totals, unused = lax.scan(one_group, initial, jnp.arange(N_DP, dtype=jnp.int32))
    return (totals[0], totals[1], totals[2], totals[3], totals[4], totals[5])
```

```python
import jax
import jax.numpy as jnp
from jax import lax
from jax.sharding import Mesh
from jax.sharding import PartitionSpec as P


DP = ("x", "zl")
HYPER = ("y", "zh", "c")
HIGHEST = lax.Precision.HIGHEST
TILE = 24


def shift(value, axis, step):
    count = lax.axis_size(axis)
    return lax.ppermute(value, axis, [(i, (i + step) % count) for i in range(count)])


def gather_near(value, axis):
    count = lax.axis_size(axis)
    return jnp.stack([value] + [shift(value, axis, -step) for step in range(1, count)])


def scatter_near(parts, axis):
    count = lax.axis_size(axis)
    total = parts[0].astype(jnp.float32)
    for step in range(1, count):
        total = total + shift(parts[step], axis, step).astype(jnp.float32)
    return total


def gather_hyper(value):
    return gather_near(gather_near(gather_near(value, "zh"), "y"), "c")


def scatter_hyper(parts):
    return scatter_near(scatter_near(scatter_near(parts, "c"), "y"), "zh")


def near_first(parts, axis):
    count = lax.axis_size(axis)
    twice = jnp.concatenate([parts, parts])
    return lax.dynamic_slice_in_dim(twice, lax.axis_index(axis), count, 0)


def in_order(parts, axis):
    count = lax.axis_size(axis)
    twice = jnp.concatenate([parts, parts])
    start = (count - lax.axis_index(axis)) % count
    return lax.dynamic_slice_in_dim(twice, start, count, 0)


def silu_slope(values):
    logistic = jax.nn.sigmoid(values)
    return logistic * (1.0 + values * (1.0 - logistic))


def class_grads(logits, slot_labels, row_count):
    largest = jnp.max(logits, axis=-1, keepdims=True)
    exponent = jnp.exp(logits - largest)
    probability = exponent / jnp.sum(exponent, axis=-1, keepdims=True)
    classes = jnp.arange(logits.shape[-1], dtype=jnp.int32)
    onehot = (slot_labels[..., None] == classes).astype(jnp.float32)
    return ((probability - onehot) / row_count).astype(jnp.bfloat16)


def pad_lanes(value):
    spare = 128 - value.shape[-1]
    return jnp.pad(value, [(0, 0)] * (value.ndim - 1) + [(0, spare)])


def picked_rows(ids, embeddings):
    select = (ids[:, None] == jnp.arange(embeddings.shape[0], dtype=ids.dtype)[None, :])
    picked = jnp.dot(
        select.astype(jnp.bfloat16), embeddings, preferred_element_type=jnp.float32
    ).astype(jnp.bfloat16)
    return select, picked


def local(
    inputs, labels, client_ids, ext_weight, ext_bias, embeddings, hyper_in, hyper_bias, hyper_out
):
    slots, rows, width_in = inputs.shape
    block, hh, classes = hyper_out.shape
    width = ext_weight.shape[1]
    hyper_size = width // block
    group = slots * hyper_size

    _, picked = picked_rows(client_ids, embeddings)
    own_hyper_preact = jnp.dot(picked, hyper_in, preferred_element_type=jnp.float32) + hyper_bias
    own_hidden = jax.nn.silu(own_hyper_preact).astype(jnp.bfloat16)

    hidden_rows = jnp.pad(pad_lanes(own_hidden), [(0, 16 - slots), (0, 0)])
    packed = jnp.concatenate([inputs.reshape(slots * rows, width_in), hidden_rows])
    gathered = gather_hyper(packed).reshape(hyper_size, slots * rows + 16, width_in)
    flat_in = gathered[:, : slots * rows].reshape(group * rows, width_in)
    hidden = gathered[:, slots * rows : slots * rows + slots, :hh].reshape(group, hh)

    column = lax.axis_index(HYPER) * block
    weight_cols = lax.dynamic_slice_in_dim(ext_weight, column, block, 1)
    bias_cols = lax.dynamic_slice_in_dim(ext_bias, column, block, 0)
    preact = jnp.dot(flat_in, weight_cols, preferred_element_type=jnp.float32) + bias_cols.astype(
        jnp.float32
    )
    features = jax.nn.silu(preact).astype(jnp.bfloat16).reshape(group, rows, block)
    heads = jnp.einsum(
        "kh,dhc->kdc", hidden, hyper_out, preferred_element_type=jnp.float32
    ).astype(jnp.bfloat16)
    logits = jnp.einsum("krd,kdc->krc", features, heads, preferred_element_type=jnp.float32)
    own_logits = scatter_hyper(logits.reshape(2, 4, 2, slots, rows, classes))
    dlogits = gather_hyper(class_grads(own_logits, labels, rows)).reshape(group, rows, classes)

    dheads = jnp.einsum(
        "krd,krc->kdc", features, dlogits, preferred_element_type=jnp.float32
    ).astype(jnp.bfloat16)

    quarter = block // 4
    ix = lax.axis_index("x")
    parts = []
    for step in range(4):
        at = ((ix + step) % 4) * quarter
        parts.append(shift(lax.dynamic_slice_in_dim(dheads, at, quarter, 1), "x", step))
    hiddens = [hidden] + [shift(hidden, "x", step) for step in range(1, 4)]
    product = sum(
        jnp.einsum("kh,kdc->dhc", h, p, preferred_element_type=jnp.float32)
        for h, p in zip(hiddens, parts)
    ).astype(jnp.bfloat16)
    grad_out = scatter_near(
        near_first(product.reshape(4, quarter // 4, hh, classes), "zl"), "zl"
    )

    dhidden = jnp.einsum("kdc,dhc->kh", dheads, hyper_out, preferred_element_type=jnp.float32)
    own_dhidden = scatter_hyper(pad_lanes(dhidden).reshape(2, 4, 2, slots, 128))
    own_dpre = own_dhidden[:, :hh] * silu_slope(own_hyper_preact)

    dfeatures = jnp.einsum(
        "krc,kdc->krd", dlogits, heads, preferred_element_type=jnp.float32
    ).astype(jnp.bfloat16)
    dpreact = (
        dfeatures.reshape(group * rows, block).astype(jnp.float32) * silu_slope(preact)
    ).astype(jnp.bfloat16)
    grad_weight = lax.dot_general(
        dpreact, flat_in, (((0,), (0,)), ((), ())), preferred_element_type=jnp.float32
    )
    grad_bias = jnp.sum(dpreact.astype(jnp.float32), axis=0)
    own = block // 16
    tiles = jnp.concatenate(
        [grad_weight.reshape(16, own, width_in), pad_lanes(grad_bias.reshape(16, 1, own))], axis=1
    ).reshape(4, 4, own + 1, width_in)
    tile = scatter_near(near_first(tiles, "x"), "x")
    tile = scatter_near(near_first(tile, "zl"), "zl")

    extra = jnp.concatenate([
        pad_lanes(own_dpre),
        pad_lanes(client_ids.astype(jnp.float32)[None]),
        jnp.zeros((TILE - own - 2 - slots, 128), jnp.float32),
    ])
    every = jnp.concatenate([tile, extra])
    for axis in ("zh", "zl", "x", "y", "c"):
        every = in_order(gather_near(every, axis), axis)
    weight_rows = every[..., :own, :].transpose(1, 4, 0, 2, 3, 5, 6).reshape(width, width_in)
    full_weight = weight_rows.T
    full_bias = every[..., own, :own].transpose(1, 4, 0, 2, 3, 5).reshape(width)
    dpre = every[..., own + 1 : own + 1 + slots, :hh].reshape(-1, hh)
    ids = every[..., own + 1 + slots, :slots].reshape(-1).astype(jnp.int32)
    select, picked = picked_rows(ids, embeddings)
    grad_in = jnp.dot(picked.astype(jnp.float32).T, dpre, precision=HIGHEST)
    grad_hbias = jnp.sum(dpre, axis=0)
    back_rows = jnp.dot(dpre, hyper_in.astype(jnp.float32).T, precision=HIGHEST)
    grad_table = jnp.dot(select.astype(jnp.float32).T, back_rows, precision=HIGHEST)
    return (full_weight, full_bias, grad_table, grad_in, grad_hbias, grad_out)


def solution(mesh):
    torus = Mesh(mesh.devices.reshape(4, 4, 4, 2, 2), DP + HYPER)
    placed = (
        P(DP + HYPER, None, None),
        P(DP + HYPER, None),
        P(DP + HYPER),
        P(),
        P(),
        P(),
        P(),
        P(),
        P(HYPER, None, None),
    )
    return jax.shard_map(
        local,
        mesh=torus,
        in_specs=placed,
        out_specs=(P(), P(), P(), P(), P(), P(HYPER + DP, None, None)),
        check_vma=False,
    )
```

```python
import jax
import jax.numpy as jnp
from jax import lax
from jax.experimental import pallas as pl
from jax.experimental.layout import Layout, with_layout_constraint
from jax.experimental.pallas import tpu as pltpu
from jax.sharding import Mesh
from jax.sharding import PartitionSpec as P


DP = ("x", "zl")
HYPER = ("y", "zh", "c")
HIGHEST = lax.Precision.HIGHEST


def shift(value, axis, step):
    count = lax.axis_size(axis)
    return lax.ppermute(value, axis, [(i, (i + step) % count) for i in range(count)])


def gather_near(value, axis):
    count = lax.axis_size(axis)
    return jnp.stack([value] + [shift(value, axis, -step) for step in range(1, count)])


def near_sum(parts):
    if len(parts) == 2:
        return parts[0] + parts[1]
    return (parts[0] + parts[2]) + (parts[1] + parts[3])


def scatter_near(parts, axis):
    return near_sum([
        (shift(parts[step], axis, step) if step else parts[0]).astype(jnp.float32)
        for step in range(lax.axis_size(axis))
    ])


def near_first(parts, axis):
    count = lax.axis_size(axis)
    twice = jnp.concatenate([parts, parts])
    return lax.dynamic_slice_in_dim(twice, lax.axis_index(axis), count, 0)


def in_order(parts, axis):
    count = lax.axis_size(axis)
    twice = jnp.concatenate([parts, parts])
    start = (count - lax.axis_index(axis)) % count
    return lax.dynamic_slice_in_dim(twice, start, count, 0)


def assemble_body(place, first, second, weight):
    zh, c = place[1], place[2]
    for block in range(8):
        at_zh, at_c, half = block // 4, (block // 2) % 2, block % 2
        at = (0, (at_zh - zh) & 1, slice(half * 128, half * 128 + 128))
        tile = jnp.where(c == at_c, first[at], second[at])
        weight[:, block * 128 : block * 128 + 128] = tile.T


def assemble(place, first, second):
    width_in, block = first.shape[-1], first.shape[-2] - 8
    half = pl.BlockSpec(
        (1, 2, block + 8, width_in), lambda g, place: ((g - place[0]) & 3, 0, 0, 0)
    )
    return pl.pallas_call(
        assemble_body,
        grid_spec=pltpu.PrefetchScalarGridSpec(
            num_scalar_prefetch=1,
            grid=(4,),
            in_specs=[half, half],
            out_specs=pl.BlockSpec((width_in, 4 * block), lambda g, place: (0, g)),
        ),
        out_shape=jax.ShapeDtypeStruct((width_in, 16 * block), jnp.float32),
        name="assemble",
    )(place, first, second)


def silu_slope(values):
    logistic = jax.nn.sigmoid(values)
    return logistic * (1.0 + values * (1.0 - logistic))


def class_grads(logits, slot_labels, row_count):
    largest = jnp.max(logits, axis=-1, keepdims=True)
    exponent = jnp.exp(logits - largest)
    probability = exponent / jnp.sum(exponent, axis=-1, keepdims=True)
    classes = jnp.arange(logits.shape[-1], dtype=jnp.int32)
    onehot = (slot_labels[..., None] == classes).astype(jnp.float32)
    return ((probability - onehot) / row_count).astype(jnp.bfloat16)


def pad_lanes(value):
    spare = 128 - value.shape[-1]
    return jnp.pad(value, [(0, 0)] * (value.ndim - 1) + [(0, spare)])


def picked_rows(ids, embeddings):
    select = (ids[:, None] == jnp.arange(embeddings.shape[0], dtype=ids.dtype)[None, :])
    picked = jnp.dot(
        select.astype(jnp.bfloat16), embeddings, preferred_element_type=jnp.float32
    ).astype(jnp.bfloat16)
    return select, picked


def hidden_grad_body(dheads, hyper_out, result):
    @pl.when(pl.program_id(0) == 0)
    def _():
        result[...] = jnp.zeros(result.shape, jnp.float32)

    total = result[...]
    for at in range(dheads.shape[0]):
        total = total + lax.dot_general(
            dheads[at], hyper_out[at], (((1,), (1,)), ((), ())), preferred_element_type=jnp.float32
        )
    result[...] = total


def hidden_grad(dheads, hyper_out):
    block, group, classes = dheads.shape
    hh = hyper_out.shape[1]
    step = 32
    return pl.pallas_call(
        hidden_grad_body,
        grid=(block // step,),
        in_specs=[
            pl.BlockSpec((step, group, classes), lambda g: (g, 0, 0)),
            pl.BlockSpec((step, hh, classes), lambda g: (g, 0, 0)),
        ],
        out_specs=pl.BlockSpec((group, hh), lambda g: (0, 0)),
        out_shape=jax.ShapeDtypeStruct((group, hh), jnp.float32),
        name="hidden_grad",
    )(dheads, hyper_out)


def sync(*values):
    return lax.optimization_barrier(values)


def hidden_layer(ids, embeddings, hyper_in, hyper_bias):
    _, picked = picked_rows(ids, embeddings)
    preact = jnp.dot(picked, hyper_in, preferred_element_type=jnp.float32) + hyper_bias
    return jax.nn.silu(preact).astype(jnp.bfloat16), preact


def local(
    inputs, labels, client_ids, ext_weight, ext_bias, embeddings, hyper_in, hyper_bias, hyper_out
):
    slots, rows, width_in = inputs.shape
    block, hh, classes = hyper_out.shape
    width = ext_weight.shape[1]
    hyper_size = width // block
    group = slots * hyper_size

    own_hidden, _ = hidden_layer(client_ids, embeddings, hyper_in, hyper_bias)

    wide_ids = client_ids[None]
    rows_after = jnp.concatenate([
        pad_lanes(own_hidden),
        pad_lanes(jnp.concatenate([wide_ids >> 8, wide_ids & 255]).astype(jnp.bfloat16)),
        jnp.zeros((12, 128), jnp.bfloat16),
    ])
    packed = jnp.concatenate([inputs.reshape(slots * rows, width_in), rows_after])
    half_packed = gather_near(packed, "zh")
    own_packed = gather_near(gather_near(half_packed, "y"), "c")
    own_packed = own_packed.reshape(hyper_size, -1, width_in)
    far_packed = gather_near(half_packed, "zl")[1:]
    far_packed = gather_near(gather_near(far_packed, "y"), "c")
    far_packed = far_packed.reshape(3 * hyper_size, -1, width_in)

    def unpacked(value):
        count = value.shape[0] * slots
        return (
            value[:, : slots * rows].reshape(count * rows, width_in),
            value[:, slots * rows : slots * rows + slots, :hh].reshape(count, hh),
        )

    column = lax.axis_index(HYPER) * block
    weight_cols = lax.dynamic_slice_in_dim(ext_weight, column, block, 1)
    bias_cols = lax.dynamic_slice_in_dim(ext_bias, column, block, 0)

    def extractor(values, weight, bias):
        preact = jnp.dot(values, weight, preferred_element_type=jnp.float32) + bias.astype(
            jnp.float32
        )
        features = jax.nn.silu(preact).astype(jnp.bfloat16)
        return preact, features.reshape(-1, rows, weight.shape[1])

    flat_in, hidden = unpacked(own_packed)
    preact, features = extractor(flat_in, weight_cols, bias_cols)
    heads = jnp.einsum(
        "kh,dhc->kdc", hidden, hyper_out, preferred_element_type=jnp.float32
    ).astype(jnp.bfloat16)
    logits = jnp.einsum("krd,kdc->krc", features, heads, preferred_element_type=jnp.float32)
    some = scatter_near(logits.reshape(2, 4, 2, slots, rows, classes), "c")
    some, turned_out = sync(some, hyper_out)
    turned_out = with_layout_constraint(turned_out, Layout(major_to_minor=(0, 1, 2)))
    some = scatter_near(some, "y")
    some, turned_out = sync(some, turned_out)
    own_logits = scatter_near(some, "zh")

    ids_rows = own_packed[:, slots * rows + slots : slots * rows + slots + 2, :slots]
    ids = ids_rows.astype(jnp.int32)
    ids = (ids[:, 0] * 256 + ids[:, 1]).reshape(group)
    _, hyper_preact = hidden_layer(ids, embeddings, hyper_in, hyper_bias)
    hyper_slope = silu_slope(hyper_preact)
    slope = silu_slope(preact)
    own_logits, hyper_slope, slope = sync(own_logits, hyper_slope, slope)

    half_dlogits = gather_near(class_grads(own_logits, labels, rows), "zh")
    far_dlogits = gather_near(half_dlogits, "zl")[1:]
    far_dlogits = gather_near(far_dlogits, "y")
    dlogits = gather_near(half_dlogits, "y")
    dlogits = gather_near(dlogits, "c").reshape(group, rows, classes)

    zl = lax.axis_index("zl")
    own = block // 16

    def share(value, dim):
        shape = value.shape
        split = value.reshape(shape[:dim] + (4, 4, own) + shape[dim + 1 :])
        picked = lax.dynamic_slice_in_dim(split, zl, 1, dim + 1)
        return picked.reshape(shape[:dim] + (4 * own,) + shape[dim + 1 :])

    dfeatures = jnp.einsum(
        "krc,kdc->krd", dlogits, heads, preferred_element_type=jnp.float32
    ).astype(jnp.bfloat16)
    dpreact = (dfeatures.reshape(group * rows, block).astype(jnp.float32) * slope).astype(
        jnp.bfloat16
    )
    grad_weight = lax.dot_general(
        dpreact, flat_in, (((0,), (0,)), ((), ())), preferred_element_type=jnp.float32
    )
    grad_bias = jnp.sum(dpreact.astype(jnp.float32), axis=0)
    tiles = jnp.concatenate(
        [grad_weight.reshape(16, own, width_in), pad_lanes(grad_bias.reshape(16, 1, own)),
         jnp.zeros((16, 7, 128), jnp.float32)], axis=1
    )
    tiles, dlogits = sync(tiles, dlogits)
    tile = lax.all_to_all(tiles, DP, split_axis=0, concat_axis=0, tiled=True)
    tile = jnp.sum(tile, axis=0)

    dheads = jnp.einsum(
        "krd,krc->kdc", features, dlogits, preferred_element_type=jnp.float32
    ).astype(jnp.bfloat16)
    turned = sync(dheads.transpose(1, 0, 2))[0]
    dhidden = hidden_grad(turned, turned_out)
    dpre = dhidden * hyper_slope
    near = jnp.concatenate([dpre, ids.astype(jnp.float32)[:, None]], axis=1)
    near = near.reshape(2, 4, 2, -1)
    near = in_order(near, "c")
    near = jnp.moveaxis(in_order(jnp.moveaxis(near, 1, 0), "y"), 0, 1)
    near = jnp.moveaxis(in_order(jnp.moveaxis(near, 2, 0), "zh"), 0, 2)
    near = pad_lanes(near.reshape(group // 2, -1))
    sent = jnp.concatenate([tile, near])
    sent = jnp.broadcast_to(sent[None], (16, *sent.shape))
    got = lax.all_to_all(sent, DP, split_axis=0, concat_axis=0, tiled=True)
    near = got[:, own + 8 :].reshape(-1, 128)
    bias_rows = jnp.pad(got[:, own, :own].reshape(block // 128, 128), [(0, 6), (0, 0)])
    every = jnp.concatenate([got[:, :own].reshape(block, 128), bias_rows])

    far_in, far_hidden = unpacked(far_packed)
    _, far_features = extractor(far_in, share(weight_cols, 1), share(bias_cols, 0))

    far_dlogits = gather_near(far_dlogits, "c").reshape(3 * group, rows, classes)

    far_dheads = jnp.einsum(
        "krd,krc->kdc", far_features, far_dlogits, preferred_element_type=jnp.float32
    ).astype(jnp.bfloat16)
    product = jnp.einsum(
        "kh,dkc->dhc",
        jnp.concatenate([hidden, far_hidden]),
        jnp.concatenate([share(turned, 0), far_dheads.transpose(1, 0, 2)], axis=1),
        preferred_element_type=jnp.float32,
    ).astype(jnp.bfloat16)
    grad_out = scatter_near(near_first(product.reshape(4, own, hh, classes), "x"), "x")

    count = near.shape[0]
    for axis in ("zh", "y"):
        both = jnp.concatenate([near, every.reshape(-1, 128)])
        both = gather_near(both, axis)
        near = near_sum(list(both[:, :count]))
        every = both[:, count:]
    near, every = sync(near, every.reshape(4, 2, block + 8, 128))
    near = near + shift(near, "c", 1)
    other = shift(every, "c", 1)

    place = jnp.stack([lax.axis_index(axis) for axis in HYPER]).astype(jnp.int32)
    full_weight = assemble(place, every, other)
    full_bias = jnp.stack([value[..., block : block + 2, :] for value in (every, other)])
    full_bias = full_bias.reshape(2, 4, 2, block)
    full_bias = in_order(full_bias, "c").transpose(1, 2, 0, 3)
    full_bias = in_order(full_bias, "y").transpose(1, 2, 0, 3)
    full_bias = in_order(full_bias, "zh").transpose(2, 0, 1, 3).reshape(width)
    near = near.reshape(-1, 128)[:, : 2 * (hh + 1)].reshape(-1, hh + 1)
    dpre = near[:, :hh]
    ids = (near[:, hh] * (1.0 / hyper_size)).astype(jnp.int32)
    select, picked = picked_rows(ids, embeddings)
    grad_in = jnp.dot(picked.astype(jnp.float32).T, dpre, precision=HIGHEST)
    grad_hbias = jnp.sum(dpre, axis=0)
    back_rows = jnp.dot(dpre, hyper_in.astype(jnp.float32).T, precision=HIGHEST)
    grad_table = jnp.dot(select.astype(jnp.float32).T, back_rows, precision=HIGHEST)
    return (full_weight, full_bias, grad_table, grad_in, grad_hbias, grad_out)


def solution(mesh):
    torus = Mesh(mesh.devices.reshape(4, 4, 4, 2, 2), DP + HYPER)
    placed = (
        P(DP + HYPER, None, None),
        P(DP + HYPER, None),
        P(DP + HYPER),
        P(),
        P(),
        P(),
        P(),
        P(),
        P(HYPER, None, None),
    )

    return jax.shard_map(
        local,
        mesh=torus,
        in_specs=placed,
        out_specs=(P(), P(), P(), P(), P(), P(HYPER + DP, None, None)),
        check_vma=False,
    )
```

```python
import jax
import jax.numpy as jnp
from jax import lax
from jax.experimental import pallas as pl
from jax.experimental.layout import Layout, with_layout_constraint
from jax.experimental.pallas import tpu as pltpu
from jax.sharding import Mesh
from jax.sharding import PartitionSpec as P


DP = ("x", "zl")
HYPER = ("y", "zh", "c")
HIGHEST = lax.Precision.HIGHEST


def shift(value, axis, step):
    count = lax.axis_size(axis)
    return lax.ppermute(value, axis, [(i, (i + step) % count) for i in range(count)])


def gather_near(value, axis):
    count = lax.axis_size(axis)
    return jnp.stack([value] + [shift(value, axis, -step) for step in range(1, count)])


def near_sum(parts):
    if len(parts) == 2:
        return parts[0] + parts[1]
    return (parts[0] + parts[2]) + (parts[1] + parts[3])


def both_cores(value):
    return value, shift(value, "c", 1)


def scatter_near(parts, axis):
    return near_sum([
        (shift(parts[step], axis, step) if step else parts[0]).astype(jnp.float32)
        for step in range(lax.axis_size(axis))
    ])


def near_first(parts, axis):
    count = lax.axis_size(axis)
    twice = jnp.concatenate([parts, parts])
    return lax.dynamic_slice_in_dim(twice, lax.axis_index(axis), count, 0)


def in_order(parts, axis):
    count = lax.axis_size(axis)
    twice = jnp.concatenate([parts, parts])
    start = (count - lax.axis_index(axis)) % count
    return lax.dynamic_slice_in_dim(twice, start, count, 0)


def assemble_body(place, first, second, weight):
    zh, c = place[1], place[2]
    for block in range(8):
        at_zh, at_c, half = block // 4, (block // 2) % 2, block % 2
        at = (0, (at_zh - zh) & 1, slice(half * 128, half * 128 + 128))
        tile = jnp.where(c == at_c, first[at].astype(jnp.float32), second[at].astype(jnp.float32))
        weight[:, block * 128 : block * 128 + 128] = tile.T


def assemble(place, first, second):
    width_in, block = first.shape[-1], first.shape[-2] - 16
    half = pl.BlockSpec(
        (1, 2, block + 16, width_in), lambda g, place: ((g - place[0]) & 3, 0, 0, 0)
    )
    return pl.pallas_call(
        assemble_body,
        grid_spec=pltpu.PrefetchScalarGridSpec(
            num_scalar_prefetch=1,
            grid=(4,),
            in_specs=[half, half],
            out_specs=pl.BlockSpec((width_in, 4 * block), lambda g, place: (0, g)),
        ),
        out_shape=jax.ShapeDtypeStruct((width_in, 16 * block), jnp.float32),
        name="assemble",
    )(place, first, second)


def silu_slope(values):
    logistic = jax.nn.sigmoid(values)
    return logistic * (1.0 + values * (1.0 - logistic))


def class_grads(logits, slot_labels, row_count):
    largest = jnp.max(logits, axis=-1, keepdims=True)
    exponent = jnp.exp(logits - largest)
    probability = exponent / jnp.sum(exponent, axis=-1, keepdims=True)
    classes = jnp.arange(logits.shape[-1], dtype=jnp.int32)
    onehot = (slot_labels[..., None] == classes).astype(jnp.float32)
    return ((probability - onehot) / row_count).astype(jnp.bfloat16)


def pad_lanes(value):
    spare = 128 - value.shape[-1]
    return jnp.pad(value, [(0, 0)] * (value.ndim - 1) + [(0, spare)])


def picked_rows(ids, embeddings):
    select = (ids[:, None] == jnp.arange(embeddings.shape[0], dtype=ids.dtype)[None, :])
    picked = jnp.dot(
        select.astype(jnp.bfloat16), embeddings, preferred_element_type=jnp.float32
    ).astype(jnp.bfloat16)
    return select, picked


def hidden_grad_body(dheads, hyper_out, result):
    @pl.when(pl.program_id(0) == 0)
    def _():
        result[...] = jnp.zeros(result.shape, jnp.float32)

    total = result[...]
    for at in range(dheads.shape[0]):
        total = total + lax.dot_general(
            hyper_out[at], dheads[at], (((1,), (1,)), ((), ())), preferred_element_type=jnp.float32
        )
    result[...] = total


def hidden_grad(dheads, hyper_out):
    block, group, classes = dheads.shape
    hh = hyper_out.shape[1]
    step = 32
    return pl.pallas_call(
        hidden_grad_body,
        grid=(block // step,),
        in_specs=[
            pl.BlockSpec((step, group, classes), lambda g: (g, 0, 0)),
            pl.BlockSpec((step, hh, classes), lambda g: (g, 0, 0)),
        ],
        out_specs=pl.BlockSpec((hh, group), lambda g: (0, 0)),
        out_shape=jax.ShapeDtypeStruct((hh, group), jnp.float32),
        name="hidden_grad",
    )(dheads, hyper_out).T


def halves(value):
    high = lax.reduce_precision(value, 8, 7)
    return high.astype(jnp.bfloat16), (value - high).astype(jnp.bfloat16)


def sync(*values):
    return lax.optimization_barrier(values)


def hidden_layer(ids, embeddings, hyper_in, hyper_bias):
    _, picked = picked_rows(ids, embeddings)
    preact = jnp.dot(picked, hyper_in, preferred_element_type=jnp.float32) + hyper_bias
    return jax.nn.silu(preact).astype(jnp.bfloat16), preact


def local(
    inputs, labels, client_ids, ext_weight, ext_bias, embeddings, hyper_in, hyper_bias, hyper_out
):
    slots, rows, width_in = inputs.shape
    block, hh, classes = hyper_out.shape
    width = ext_weight.shape[1]
    hyper_size = width // block
    group = slots * hyper_size

    own_hidden, _ = hidden_layer(client_ids, embeddings, hyper_in, hyper_bias)

    wide_ids = client_ids[None]
    rows_after = jnp.concatenate([
        pad_lanes(own_hidden),
        pad_lanes(jnp.concatenate([wide_ids >> 8, wide_ids & 255]).astype(jnp.bfloat16)),
        jnp.zeros((12, 128), jnp.bfloat16),
    ])
    packed = jnp.concatenate([inputs.reshape(slots * rows, width_in), rows_after])
    half_packed = gather_near(packed, "zh")
    own_packed = gather_near(gather_near(half_packed, "y"), "c")
    own_packed = own_packed.reshape(hyper_size, -1, width_in)
    far_packed = gather_near(half_packed, "zl")[1:]
    far_packed = both_cores(gather_near(far_packed, "y"))

    def unpacked(value):
        count = value.shape[0] * slots
        return (
            value[:, : slots * rows].reshape(count * rows, width_in),
            value[:, slots * rows : slots * rows + slots, :hh].reshape(count, hh),
        )

    column = lax.axis_index(HYPER) * block
    weight_cols = lax.dynamic_slice_in_dim(ext_weight, column, block, 1)
    bias_cols = lax.dynamic_slice_in_dim(ext_bias, column, block, 0)

    def extractor(values, weight, bias):
        preact = jnp.dot(values, weight, preferred_element_type=jnp.float32) + bias.astype(
            jnp.float32
        )
        features = jax.nn.silu(preact).astype(jnp.bfloat16)
        return preact, features.reshape(-1, rows, weight.shape[1])

    flat_in, hidden = unpacked(own_packed)
    preact, features = extractor(flat_in, weight_cols, bias_cols)
    heads = jnp.einsum(
        "kh,dhc->kdc", hidden, hyper_out, preferred_element_type=jnp.float32
    ).astype(jnp.bfloat16)
    logits = jnp.einsum("krd,kdc->krc", features, heads, preferred_element_type=jnp.float32)
    some = scatter_near(logits.reshape(2, 4, 2, slots, rows, classes), "c")
    some, turned_out = sync(some, hyper_out)
    turned_out = with_layout_constraint(turned_out, Layout(major_to_minor=(0, 1, 2)))
    some = scatter_near(some, "y")
    some, turned_out = sync(some, turned_out)
    own_logits = scatter_near(some, "zh")

    ids_rows = own_packed[:, slots * rows + slots : slots * rows + slots + 2, :slots]
    ids = ids_rows.astype(jnp.int32)
    ids = (ids[:, 0] * 256 + ids[:, 1]).reshape(group)
    _, hyper_preact = hidden_layer(ids, embeddings, hyper_in, hyper_bias)
    hyper_slope = silu_slope(hyper_preact)
    slope = silu_slope(preact)
    own_logits, hyper_slope, slope = sync(own_logits, hyper_slope, slope)

    zl = lax.axis_index("zl")
    own = block // 16

    def share(value, dim):
        shape = value.shape
        split = value.reshape(shape[:dim] + (4, 4, own) + shape[dim + 1 :])
        picked = lax.dynamic_slice_in_dim(split, zl, 1, dim + 1)
        return picked.reshape(shape[:dim] + (4 * own,) + shape[dim + 1 :])

    half_dlogits = gather_near(class_grads(own_logits, labels, rows), "zh")
    far_dlogits = gather_near(half_dlogits, "zl")[1:]
    far_dlogits = gather_near(far_dlogits, "y")
    dlogits = gather_near(half_dlogits, "y")

    def far_extractor(packed):
        far_in, far_hidden = unpacked(packed.reshape(3 * hyper_size // 2, -1, width_in))
        _, far_features = extractor(far_in, share(weight_cols, 1), share(bias_cols, 0))
        return far_features, far_hidden

    near_core = far_extractor(far_packed[0])
    dlogits, near_core = sync(dlogits, near_core)
    dlogits = gather_near(dlogits, "c").reshape(group, rows, classes)

    dfeatures = jnp.einsum(
        "krc,kdc->krd", dlogits, heads, preferred_element_type=jnp.float32
    ).astype(jnp.bfloat16)
    dpreact = (dfeatures.reshape(group * rows, block).astype(jnp.float32) * slope).astype(
        jnp.bfloat16
    )
    grad_weight = lax.dot_general(
        dpreact, flat_in, (((0,), (0,)), ((), ())), preferred_element_type=jnp.float32
    )
    grad_bias = jnp.sum(dpreact.astype(jnp.float32), axis=0)
    tiles = jnp.concatenate(
        [grad_weight.reshape(16, own, width_in),
         jnp.broadcast_to(grad_bias.reshape(1, block // 128, 128), (16, block // 128, 128)),
         jnp.zeros((16, 8 - block // 128, 128), jnp.float32)], axis=1
    )
    tiles, dlogits = sync(tiles, dlogits)
    tile = lax.all_to_all(tiles, DP, split_axis=0, concat_axis=0, tiled=True)
    tile = jnp.sum(tile, axis=0)

    dheads = jnp.einsum(
        "krd,krc->kdc", features, dlogits, preferred_element_type=jnp.float32
    ).astype(jnp.bfloat16)
    turned = sync(dheads.transpose(1, 0, 2))[0]
    dhidden = hidden_grad(turned, turned_out)
    dpre = dhidden * hyper_slope
    near = jnp.concatenate([dpre, ids.astype(jnp.float32)[:, None]], axis=1)
    near = near.reshape(2, 4, 2, -1)
    near = in_order(near, "c")
    near = jnp.moveaxis(in_order(jnp.moveaxis(near, 1, 0), "y"), 0, 1)
    near = jnp.moveaxis(in_order(jnp.moveaxis(near, 2, 0), "zh"), 0, 2)
    near = pad_lanes(near.reshape(group // 2, -1))
    sent = jnp.concatenate([tile, near])
    sent = jnp.broadcast_to(sent[None], (16, *sent.shape))
    got = lax.all_to_all(sent, DP, split_axis=0, concat_axis=0, tiled=True)
    near = got[:, own + 8 :].reshape(-1, 128)
    bias_rows = jnp.pad(tile[own:], [(0, 8), (0, 0)])
    every = jnp.concatenate([got[:, :own].reshape(block, 128), bias_rows])

    far_dlogits = both_cores(far_dlogits)
    hiddens, all_dheads = [hidden], [share(turned, 0)]
    cores = (near_core, far_extractor(far_packed[1]))
    for (far_features, far_hidden), core_dlogits in zip(cores, far_dlogits):
        far_dheads = jnp.einsum(
            "krd,krc->kdc",
            far_features,
            core_dlogits.reshape(3 * group // 2, rows, classes),
            preferred_element_type=jnp.float32,
        ).astype(jnp.bfloat16)
        hiddens.append(far_hidden)
        all_dheads.append(far_dheads.transpose(1, 0, 2))

    product = jnp.einsum(
        "kh,dkc->dhc",
        jnp.concatenate(hiddens),
        jnp.concatenate(all_dheads, axis=1),
        preferred_element_type=jnp.float32,
    ).astype(jnp.bfloat16)
    grad_out = scatter_near(near_first(product.reshape(4, own, hh, classes), "x"), "x")

    count = near.shape[0]
    every = every.astype(jnp.bfloat16)
    near = near + shift(near, "c", 1)
    for axis in ("zh", "y"):
        both = jnp.concatenate([*halves(near), every.reshape(-1, 128)])
        both = gather_near(both, axis)
        near = near_sum([
            high.astype(jnp.float32) + low.astype(jnp.float32)
            for high, low in zip(both[:, :count], both[:, count : 2 * count])
        ])
        every = both[:, 2 * count :]
    every = every.reshape(4, 2, -1, 128)
    other = shift(every, "c", 1)

    place = jnp.stack([lax.axis_index(axis) for axis in HYPER]).astype(jnp.int32)
    full_weight = assemble(place, every, other)
    full_bias = jnp.stack([value[..., block : block + 2, :] for value in (every, other)])
    full_bias = full_bias.astype(jnp.float32).reshape(2, 4, 2, block)
    full_bias = in_order(full_bias, "c").transpose(1, 2, 0, 3)
    full_bias = in_order(full_bias, "y").transpose(1, 2, 0, 3)
    full_bias = in_order(full_bias, "zh").transpose(2, 0, 1, 3).reshape(width)
    near = near.reshape(-1, 128)[:, : 2 * (hh + 1)].reshape(-1, hh + 1)
    dpre = near[:, :hh]
    ids = (near[:, hh] * (1.0 / hyper_size)).astype(jnp.int32)
    select, picked = picked_rows(ids, embeddings)
    grad_in = jnp.dot(picked.astype(jnp.float32).T, dpre, precision=HIGHEST)
    grad_hbias = jnp.sum(dpre, axis=0)
    back_rows = jnp.dot(dpre, hyper_in.astype(jnp.float32).T, precision=HIGHEST)
    grad_table = jnp.dot(select.astype(jnp.float32).T, back_rows, precision=HIGHEST)
    return (full_weight, full_bias, grad_table, grad_in, grad_hbias, grad_out)


def solution(mesh):
    torus = Mesh(mesh.devices.reshape(4, 4, 4, 2, 2), DP + HYPER)
    placed = (
        P(DP + HYPER, None, None),
        P(DP + HYPER, None),
        P(DP + HYPER),
        P(),
        P(),
        P(),
        P(),
        P(),
        P(HYPER, None, None),
    )

    return jax.shard_map(
        local,
        mesh=torus,
        in_specs=placed,
        out_specs=(P(), P(), P(), P(), P(), P(HYPER + DP, None, None)),
        check_vma=False,
    )
```
